256 devices in a mesh: band: 64 (over x, z_lo, y, core), pw: 4 (over z_hi).
Axes of the slice: x: 4, y: 4, z: 8 (z_hi: 4, z_lo: 2; z = z_hi * 2 + z_lo), core: 2. Of those that a mesh axis runs over, the one named last changes fastest.
Arguments:
- pair_density: bfloat16 [320, 128, 9216], P('band', None, 'pw'), may hold values from -6 to 6
- eigvecs: bfloat16 [2944, 9216], P('band', 'pw'), may hold values from -0.0625 to 0.0625
- screening: bfloat16 [2944, 2944], P('pw'), may hold values from -0.00048828125 to 0.00048828125
- occupation: float32 [128], replicated, may hold values from 0 to 1
- window_start: int32 [320], P('band'), may hold values from 0 to 511, as said below
- window_len: int32 [320], P('band'), may hold values from 1 to 128, as said below
- slot_band: int32 [320], P('band'), may hold values from -1 to 127, as said below
Outputs:
- sigma: float32 [512, 512], P(('band', 'pw'))
The draws below stay inside these ranges and needn't reach their ends.
Inputs may be any that keep to these rules, and one draw needn't show every extreme that they name: window_start + window_len <= 512 for every slot. `window_len`: some slot has a window of 128 bands. On each index of band the live slots (slot_band >= 0) come first among its 5 slots; each index holds 3 to 5 live slots, and the counts of index i and index i + 64 / 2 add up to 8.
All inputs are finite; a program needn't handle non-finite values.
Results may differ from the reference program's by a relative error of at most 0.0049.
Values may be sent and summed in bfloat16 or wider, within the bound.
No kernel may reach another device: no remote copies, remote signals or barrier semaphores. Data moves between devices by JAX's collectives and lax.ppermute only.
A program may use at most 128 MiB of HBM per device.

```python
import jax
import jax.numpy as jnp
from jax import lax

NB_SIGMA = 512
BLOCK = 128
G = 9216
S = 2944
CAP = 5
SLOTS = 320
NSUM = 128


def window_parts(key):
    lengths = jax.random.randint(jax.random.fold_in(key, 11), (SLOTS,), 1, BLOCK + 1)
    lengths = lengths.at[0].set(BLOCK)
    lengths = lengths.at[1].set(1)
    spaces = NB_SIGMA - lengths + 1
    raw_bits = jax.random.randint(jax.random.fold_in(key, 12), (SLOTS,), 0, 1 << 30)
    starts = raw_bits % spaces
    starts = starts.at[0].set(0)
    starts = starts.at[1].set(NB_SIGMA - 1)
    return (starts.astype(jnp.int32), lengths.astype(jnp.int32))


def draw_window_start(key, part):
    starts, lengths = window_parts(key)
    return starts


def draw_window_len(key, part):
    starts, lengths = window_parts(key)
    return lengths


def draw_slot_band(key, part):
    groups = SLOTS // CAP
    halves = groups // 2
    lower = jax.random.randint(jax.random.fold_in(key, 21), (halves,), CAP - 2, CAP + 1)
    counts = jnp.concatenate([lower, 2 * CAP - 2 - lower])
    position = jnp.arange(SLOTS, dtype=jnp.int32) % CAP
    device = jnp.arange(SLOTS, dtype=jnp.int32) // CAP
    band_ids = jax.random.randint(jax.random.fold_in(key, 22), (SLOTS,), 0, NSUM)
    return jnp.where(position < counts[device], band_ids, -1).astype(jnp.int32)


def steps_of(own_key, extent, pieces, least, top_value):
    def one(axis_at, parts):
        heights = jax.random.uniform(jax.random.fold_in(jax.random.fold_in(own_key, 6), axis_at), (parts,), jnp.float32, least / len(pieces), top_value / len(pieces))
        return jnp.repeat(jnp.exp(heights), extent[axis_at] // parts).reshape((-1,) + (1,) * (len(extent) - axis_at - 1))

    level = one(*pieces[0])
    for cut in pieces[1:]:
        level = level * one(*cut)
    return level


def noise(own_key, shape, width, bound, pieces=(), kind=jnp.bfloat16):
    result = jax.random.normal(own_key, shape, jnp.float32) * width
    if len(pieces) > 0:
        result = steps_of(own_key, shape, pieces, -0.22, 0.18) * result
    return jnp.clip(result, min=-bound, max=bound).astype(kind)


def setup_inputs(seed: int = 0) -> dict:
    streams_of = jax.random.split(jax.random.key(seed), 8)
    return {
        "pair_density": noise(streams_of[0], (SLOTS, BLOCK, G), 1.0, 6.0, ((0, 64), (2, 4))),
        "eigvecs": noise(streams_of[1], (S, G), G ** -0.5, 0.0625, ((0, 64), (1, 4))),
        "screening": noise(streams_of[2], (S, S), (16 * S * S) ** -0.5, 0.00048828125, ((0, 4),)),
        "occupation": jnp.clip(jax.random.uniform(streams_of[3], (NSUM,), jnp.float32, 0.0, 1.0), 0.0, 1.0),
        "window_start": draw_window_start(jax.random.fold_in(streams_of[7], 71), 0),
        "window_len": draw_window_len(jax.random.fold_in(streams_of[7], 71), 0),
        "slot_band": draw_slot_band(jax.random.fold_in(streams_of[7], 71), 0),
    }


def reference(pair_density, eigvecs, screening, occupation, window_start, window_len, slot_band):
    row_ids = jnp.arange(BLOCK, dtype=jnp.int32)
    band_list = jnp.arange(NSUM, dtype=jnp.int32)

    def add_slot(totals, item):
        density, offset, length, band_id = item
        raw_proj = jnp.dot(density, eigvecs.T, preferred_element_type=jnp.float32)
        keep_rows = ((row_ids < length) & (band_id >= 0)).astype(jnp.float32)
        projected = (raw_proj * keep_rows[:, None]).astype(jnp.bfloat16)
        screened = jnp.dot(projected, screening.T, preferred_element_type=jnp.float32).astype(jnp.bfloat16)
        block_sigma = jnp.dot(screened, projected.T, preferred_element_type=jnp.float32)
        weight = 0.5 - jnp.sum(jnp.where(band_list == band_id, occupation, jnp.zeros_like(occupation)))
        first = offset.astype(jnp.int32)
        previous = lax.dynamic_slice(totals, (first, first), (BLOCK, BLOCK))
        totals = lax.dynamic_update_slice(totals, previous + weight * block_sigma, (first, first))
        return totals, None

    start_sum = jnp.zeros((NB_SIGMA + BLOCK, NB_SIGMA + BLOCK), jnp.float32)
    totals, unused = lax.scan(add_slot, start_sum, (pair_density, window_start, window_len, slot_band))
    return totals[:NB_SIGMA, :NB_SIGMA]
```

```python
import jax
import jax.numpy as jnp
from jax import lax
from jax.sharding import PartitionSpec as P


NB_SIGMA = 512
PAD = 48
OFFSETS = (0, 3, 1, 2)


def place(band):
    return band >> 4, (band >> 3) & 1, (band >> 1) & 3, band & 1


def band_of(x, zl, y, core):
    return ((x * 2 + zl) * 4 + y) * 2 + core


def moved_in_plane(band, along_first, step):
    x, zl, y, core = place(band)
    if (core == 0) == along_first:
        x = (x + step) % 4
    else:
        y = (y + step) % 4
    return band_of(x, zl, y, core)


def plane_step(array, along_first, step):
    return lax.ppermute(
        array, "band", [(i, moved_in_plane(i, along_first, step)) for i in range(64)]
    )


def flipped(array, bit):
    return lax.ppermute(array, "band", [(i, i ^ (1 << bit)) for i in range(64)])


def ring(array, step):
    return lax.ppermute(array, "pw", [(i, (i + step) % 4) for i in range(4)])


def line_of(block):
    two = plane_step(block, True, 2)
    minus = plane_step(block, True, -1)
    plus = plane_step(block, True, 1)
    return block, plus, minus, two


def in_rows(rows, width):
    left = rows[:, width:]
    eights = [left[i : i + 8] for i in range(0, rows.shape[0], 8)]
    tail = jnp.concatenate(eights, 1)
    tail = jnp.pad(tail, ((0, 0), (0, width - tail.shape[1])))
    return jnp.concatenate([rows[:, :width], tail], 0)


def out_of_rows(packed, count, extra):
    groups = count // 8
    tail = jnp.concatenate(
        [packed[:, None, count:, i * extra : (i + 1) * extra] for i in range(groups)], 1
    )
    main = packed[:, :count]
    return jnp.concatenate(
        [main.reshape(-1, packed.shape[2]), tail.reshape(-1, extra)], 1
    )


def paired(array, which, second):
    pairs = []
    for band in range(64):
        for pw in range(4):
            even_pairs = (((band & 1) ^ which) == 0) != second
            other = pw ^ 1 if even_pairs else (pw + 1 if pw % 2 else pw - 1) % 4
            pairs.append((band * 4 + pw, band * 4 + other))
    return lax.ppermute(array, ("band", "pw"), pairs)


def rows_to_owner(rows, me, core):
    first = jnp.where(core == 0, me ^ 1, jnp.where(me % 2 == 1, (me + 1) % 4, (me + 3) % 4))
    second = jnp.where(core == 0, jnp.where(me % 2 == 1, (me + 1) % 4, (me + 3) % 4), me ^ 1)

    def at(k):
        return lax.dynamic_index_in_dim(rows, k, 0, keepdims=False)

    opposite = (me + 2) % 4
    got = paired(jnp.stack([at(first), at(opposite)]), 0, False)
    own, passed = at(me) + got[0], at(second) + got[1]
    return own + paired(passed, 0, True)


def column_rows(x, zl, y, core, rows_each):
    col = jnp.arange(32 * PAD, dtype=jnp.int32)
    second, first = chosen(col // (8 * PAD), OFFSETS), chosen((col // (2 * PAD)) % 4, OFFSETS)
    other_z, r = (col // PAD) % 2, col % PAD
    cx = (x + jnp.where(core == 0, first, second)) % 4
    cy = (y + jnp.where(core == 0, second, first)) % 4
    band = band_of(cx, zl ^ other_z, cy, core)
    return jnp.where(r < rows_each, band * rows_each + r, -1)


def chosen(index, values):
    out = jnp.zeros_like(index)
    for i, v in enumerate(values):
        if v:
            out = jnp.where(index == i, v, out)
    return out


def body(pair_density, eigvecs, screening, occupation, window_start, window_len, slot_band):
    capacity, block, planes = pair_density.shape
    rows_each = eigvecs.shape[0]
    basis = screening.shape[1]
    bf16, f32 = jnp.bfloat16, jnp.float32
    nt = (((1,), (1,)), ((), ()))
    me = lax.axis_index("pw")
    x, zl, y, core = place(lax.axis_index("band"))
    last = capacity - 1
    row_ids = jnp.arange(block, dtype=jnp.int32)

    keep = (row_ids[None, :] < window_len[:, None]) & (slot_band[:, None] >= 0)
    spare = jnp.where(keep[last][:, None], pair_density[last], 0)
    got_block = flipped(spare, 5)
    taking = jnp.sum((slot_band >= 0).astype(jnp.int32)) == capacity - 2
    kept = jnp.where(keep[: last - 1, :, None], pair_density[: last - 1], 0)
    fourth = jnp.where(taking, got_block, jnp.where(keep[last - 1][:, None], pair_density[last - 1], 0))
    own_slots = jnp.concatenate([kept, fourth[None]], 0)
    other_slots = flipped(own_slots, 0)
    flat = jnp.concatenate([own_slots, other_slots], 0).reshape(8 * block, planes)

    width = screening.shape[0]
    half = width // 2
    sixteenth = half // 16
    own_start = jnp.where(core == 0, 0, width - 384)
    own_rows = lax.optimization_barrier(lax.dynamic_slice_in_dim(screening, own_start, 384, 0))
    away = lax.dynamic_slice_in_dim(screening, core * half + (x * 4 + y) * sixteenth, sixteenth, 0)
    away = ring(jnp.pad(away, ((0, 24 - sixteenth), (0, 0))), 2)

    to_pad = ((0, PAD - rows_each), (0, 0))
    lower = flipped(eigvecs, 3)
    mine = jnp.concatenate(
        [jnp.pad(eigvecs, to_pad), jnp.pad(lower, to_pad), in_rows(away, planes)], 0
    )
    line = line_of(mine)
    message = jnp.concatenate([b[: 2 * PAD] for b in line] + [b[2 * PAD :] for b in line], 0)
    below, above = plane_step(message, False, 1), plane_step(message, False, -1)
    far = (plane_step(below[:256], False, 1), plane_step(above[256:], False, -1))
    chunks = (
        (message, 384),
        (jnp.concatenate([below[:384], above[:384]], 0), 768),
        (jnp.concatenate([far[0], far[1][:128]], 0), 384),
    )
    away_rows = jnp.concatenate([message[384:], below[384:], above[384:], far[1][128:]], 0)
    away_rows = out_of_rows(away_rows.reshape(16, 32, planes), 24, basis - planes)
    at = jnp.arange(384, dtype=jnp.int32)
    second, first, r = chosen(at // 96, OFFSETS), chosen((at // 24) % 4, OFFSETS), at % 24
    cx = (x + jnp.where(core == 0, first, second)) % 4
    cy = (y + jnp.where(core == 0, second, first)) % 4
    away_ids = ((me + 2) % 4) * width + core * half + (cx * 4 + cy) * sixteenth + r
    away_ids = jnp.where(r < sixteenth, away_ids, -2)
    own_ids = own_start + jnp.arange(384, dtype=jnp.int32)
    own_ids = jnp.where(own_ids // half == core, me * width + own_ids, -2)
    row_list = jnp.concatenate([own_ids, away_ids])
    col_list = jnp.concatenate(
        [column_rows(x, zl, y, core, rows_each), column_rows(x, zl, y, 1 - core, rows_each)]
    )

    def spread_out(rows):
        cols = lax.optimization_barrier(col_list)
        spread = (jnp.arange(basis, dtype=jnp.int32)[:, None] == cols[None, :]).astype(bf16)
        out = lax.dot_general(
            rows, spread, (((1,), (0,)), ((), ())), preferred_element_type=f32
        )
        return lax.optimization_barrier(out.astype(bf16))

    screens = (spread_out(own_rows), spread_out(away_rows))
    pick = (row_list[:, None] == col_list[None, :]).astype(bf16)

    sets = [core, 1 - core]
    low = [jnp.where(s == 0, (me == 0) | (me == 3), me < 2) for s in sets]
    own_cols = []
    for rows, count in chunks:
        part = lax.dot_general(flat, rows, nt, preferred_element_type=f32)
        part = part.reshape(2, 4, block, part.shape[1])[:, :, :, :count]
        summed = []
        for i in range(2):

            def two_slots(start):
                return lax.dynamic_slice_in_dim(part[i], start, 2, 0)

            give = two_slots(jnp.where(low[i], 2, 0)).astype(bf16)
            take = two_slots(jnp.where(low[i], 0, 2))
            two = take + paired(give, i, False).astype(f32)
            four = two + paired(two.astype(bf16), i, True).astype(f32)
            summed.append(four.astype(bf16))
        own_cols.append(jnp.concatenate(summed, 0))
    own_cols = jnp.concatenate(own_cols, 2)
    other_cols = flipped(own_cols, 0)
    projected = jnp.concatenate(
        [own_cols, jnp.concatenate([other_cols[2:], other_cols[:2]], 0)], 2
    )

    flat_proj = projected.reshape(4 * block, -1)
    screened = [lax.dot_general(flat_proj, m, nt, preferred_element_type=f32) for m in screens]
    picked = lax.dot_general(flat_proj, pick, nt, preferred_element_type=f32).astype(bf16)
    batched = (((2,), (2,)), ((0,), (0,)))

    def two_parts(a):
        high = lax.reduce_precision(a, 8, 7)
        return high.astype(bf16), (a - high).astype(bf16)

    block_sigma = sum(
        lax.dot_general(
            part.reshape(4, block, -1),
            picked[:, i * 384 : (i + 1) * 384].reshape(4, block, -1),
            batched,
            preferred_element_type=f32,
        )
        for i, s in enumerate(screened)
        for part in two_parts(s)
    )

    spare_meta = jnp.stack([window_start[last], slot_band[last]])
    got_meta = flipped(spare_meta, 5)
    own_meta = jnp.stack([window_start[:last], slot_band[:last]])
    is_last = jnp.arange(last)[None, :] == last - 1
    meta = jnp.where(is_last & taking, got_meta[:, None], own_meta)
    other_meta = flipped(meta, 0)
    four_meta = jnp.concatenate(
        [
            lax.dynamic_slice_in_dim(m, jnp.where(low[i], 0, 2), 2, 1)
            for i, m in enumerate((meta, other_meta))
        ],
        1,
    )
    starts, band_ids = four_meta[0], four_meta[1]
    band_list = jnp.arange(occupation.shape[0], dtype=jnp.int32)
    weights = 0.5 - jnp.sum(
        jnp.where(band_list[None, :] == band_ids[:, None], occupation[None, :], 0.0), axis=1
    )
    weighted = block_sigma * weights[:, None, None]
    place_rows = (
        jnp.arange(NB_SIGMA, dtype=jnp.int32)[None, :, None] == (starts[:, None] + row_ids)[:, None, :]
    ).astype(bf16)
    sigma_part = sum(
        lax.dot_general(
            lax.dot_general(
                place_rows, w, (((2,), (1,)), ((0,), (0,))), preferred_element_type=f32
            ).astype(bf16),
            place_rows,
            (((0, 2), (0, 2)), ((), ())),
            preferred_element_type=f32,
        )
        for w in two_parts(weighted)
    )
    by_band = lax.all_to_all(
        sigma_part.astype(bf16).reshape(64, 8, NB_SIGMA), "band", 0, 0, tiled=True
    )
    rows = jnp.sum(by_band.astype(f32), axis=0).reshape(4, 2, NB_SIGMA)
    return rows_to_owner(rows, me, core)


def solution(mesh):
    return jax.shard_map(
        body,
        mesh=mesh,
        in_specs=(
            P("band", None, "pw"),
            P("band", "pw"),
            P("pw", None),
            P(),
            P("band"),
            P("band"),
            P("band"),
        ),
        out_specs=P(("band", "pw"), None),
        check_vma=False,
    )
```

```python
import jax
import jax.numpy as jnp
from jax import lax
from jax.sharding import PartitionSpec as P


NB_SIGMA = 512
PAD = 48
OFFSETS = (0, 3, 1, 2)


def place(band):
    return band >> 4, (band >> 3) & 1, (band >> 1) & 3, band & 1


def band_of(x, zl, y, core):
    return ((x * 2 + zl) * 4 + y) * 2 + core


def moved_in_plane(band, along_first, step):
    x, zl, y, core = place(band)
    if (core == 0) == along_first:
        x = (x + step) % 4
    else:
        y = (y + step) % 4
    return band_of(x, zl, y, core)


def plane_step(array, along_first, step):
    return lax.ppermute(
        array, "band", [(i, moved_in_plane(i, along_first, step)) for i in range(64)]
    )


def flipped(array, bit):
    return lax.ppermute(array, "band", [(i, i ^ (1 << bit)) for i in range(64)])


def ring(array, step):
    return lax.ppermute(array, "pw", [(i, (i + step) % 4) for i in range(4)])


def line_of(block):
    two = plane_step(block, True, 2)
    minus = plane_step(block, True, -1)
    plus = plane_step(block, True, 1)
    return block, plus, minus, two


def in_rows(rows, width):
    left = rows[:, width:]
    eights = [left[i : i + 8] for i in range(0, rows.shape[0], 8)]
    tail = jnp.concatenate(eights, 1)
    tail = jnp.pad(tail, ((0, 0), (0, width - tail.shape[1])))
    return jnp.concatenate([rows[:, :width], tail], 0)


def out_of_rows(packed, count, extra):
    groups = count // 8
    tail = jnp.concatenate(
        [packed[:, None, count:, i * extra : (i + 1) * extra] for i in range(groups)], 1
    )
    main = packed[:, :count]
    return jnp.concatenate(
        [main.reshape(-1, packed.shape[2]), tail.reshape(-1, extra)], 1
    )


def paired(array, which, second):
    pairs = []
    for band in range(64):
        for pw in range(4):
            even_pairs = (((band & 1) ^ which) == 0) != second
            other = pw ^ 1 if even_pairs else (pw + 1 if pw % 2 else pw - 1) % 4
            pairs.append((band * 4 + pw, band * 4 + other))
    return lax.ppermute(array, ("band", "pw"), pairs)


def rows_to_owner(rows, me, core):
    first = jnp.where(core == 0, me ^ 1, jnp.where(me % 2 == 1, (me + 1) % 4, (me + 3) % 4))
    second = jnp.where(core == 0, jnp.where(me % 2 == 1, (me + 1) % 4, (me + 3) % 4), me ^ 1)

    def at(k):
        return lax.dynamic_index_in_dim(rows, k, 0, keepdims=False)

    opposite = (me + 2) % 4
    got = paired(jnp.stack([at(first), at(opposite)]), 0, False)
    own, passed = at(me) + got[0], at(second) + got[1]
    return own + paired(passed, 0, True)


def column_rows(x, zl, y, core, rows_each):
    col = jnp.arange(32 * PAD, dtype=jnp.int32)
    second, first = chosen(col // (8 * PAD), OFFSETS), chosen((col // (2 * PAD)) % 4, OFFSETS)
    other_z, r = (col // PAD) % 2, col % PAD
    cx = (x + jnp.where(core == 0, first, second)) % 4
    cy = (y + jnp.where(core == 0, second, first)) % 4
    band = band_of(cx, zl ^ other_z, cy, core)
    return jnp.where(r < rows_each, band * rows_each + r, -1)


def chosen(index, values):
    out = jnp.zeros_like(index)
    for i, v in enumerate(values):
        if v:
            out = jnp.where(index == i, v, out)
    return out


def body(pair_density, eigvecs, screening, occupation, window_start, window_len, slot_band):
    capacity, block, planes = pair_density.shape
    rows_each = eigvecs.shape[0]
    basis = screening.shape[1]
    bf16, f32 = jnp.bfloat16, jnp.float32
    nt = (((1,), (1,)), ((), ()))
    me = lax.axis_index("pw")
    x, zl, y, core = place(lax.axis_index("band"))
    last = capacity - 1
    row_ids = jnp.arange(block, dtype=jnp.int32)

    keep = (row_ids[None, :] < window_len[:, None]) & (slot_band[:, None] >= 0)
    spare = jnp.where(keep[last][:, None], pair_density[last], 0)
    got_block = flipped(spare, 5)
    taking = jnp.sum((slot_band >= 0).astype(jnp.int32)) == capacity - 2
    kept = jnp.where(keep[: last - 1, :, None], pair_density[: last - 1], 0)
    fourth = jnp.where(taking, got_block, jnp.where(keep[last - 1][:, None], pair_density[last - 1], 0))
    own_slots = jnp.concatenate([kept, fourth[None]], 0)
    other_slots = flipped(own_slots, 0)
    flat = jnp.concatenate([own_slots, other_slots], 0).reshape(8 * block, planes)

    width = screening.shape[0]
    half = width // 2
    sixteenth = half // 16
    own_start = jnp.where(core == 0, 0, width - 384)
    own_rows = lax.optimization_barrier(lax.dynamic_slice_in_dim(screening, own_start, 384, 0))
    away = lax.dynamic_slice_in_dim(screening, core * half + (x * 4 + y) * sixteenth, sixteenth, 0)
    away = ring(jnp.pad(away, ((0, 24 - sixteenth), (0, 0))), 2)

    to_pad = ((0, PAD - rows_each), (0, 0))
    lower = flipped(eigvecs, 3)
    mine = jnp.concatenate(
        [jnp.pad(eigvecs, to_pad), jnp.pad(lower, to_pad), in_rows(away, planes)], 0
    )
    line = line_of(mine)
    message = jnp.concatenate([b[: 2 * PAD] for b in line] + [b[2 * PAD :] for b in line], 0)
    below, above = plane_step(message, False, 1), plane_step(message, False, -1)
    far = (plane_step(below[:256], False, 1), plane_step(above[256:], False, -1))
    chunks = (((message, 384),), ((below, 384), (above, 384)), ((far[0], 256), (far[1], 128)))
    away_rows = jnp.concatenate([message[384:], below[384:], above[384:], far[1][128:]], 0)
    away_rows = out_of_rows(away_rows.reshape(16, 32, planes), 24, basis - planes)
    at = jnp.arange(384, dtype=jnp.int32)
    second, first, r = chosen(at // 96, OFFSETS), chosen((at // 24) % 4, OFFSETS), at % 24
    cx = (x + jnp.where(core == 0, first, second)) % 4
    cy = (y + jnp.where(core == 0, second, first)) % 4
    away_ids = ((me + 2) % 4) * width + core * half + (cx * 4 + cy) * sixteenth + r
    away_ids = jnp.where(r < sixteenth, away_ids, -2)
    own_ids = own_start + jnp.arange(384, dtype=jnp.int32)
    own_ids = jnp.where(own_ids // half == core, me * width + own_ids, -2)
    row_list = jnp.concatenate([own_ids, away_ids])
    col_list = jnp.concatenate(
        [column_rows(x, zl, y, core, rows_each), column_rows(x, zl, y, 1 - core, rows_each)]
    )

    def spread_out(rows):
        cols = lax.optimization_barrier(col_list)
        spread = (jnp.arange(basis, dtype=jnp.int32)[:, None] == cols[None, :]).astype(bf16)
        out = lax.dot_general(
            rows, spread, (((1,), (0,)), ((), ())), preferred_element_type=f32
        )
        return lax.optimization_barrier(out.astype(bf16))

    screens = (spread_out(own_rows), spread_out(away_rows))
    pick = (row_list[:, None] == col_list[None, :]).astype(bf16)

    sets = [core, 1 - core]
    low = [jnp.where(s == 0, (me == 0) | (me == 3), me < 2) for s in sets]
    own_cols, other_cols = [], []
    for pieces in chunks:
        parts = []
        for rows, count in pieces:
            part = lax.dot_general(flat, rows, nt, preferred_element_type=f32)
            parts.append(part.reshape(2, 4, block, part.shape[1])[:, :, :, :count])
        summed = []
        for i in range(2):

            def two_slots(start):
                return jnp.concatenate(
                    [lax.dynamic_slice_in_dim(part[i], start, 2, 0) for part in parts], 2
                )

            give = two_slots(jnp.where(low[i], 2, 0)).astype(bf16)
            take = two_slots(jnp.where(low[i], 0, 2))
            two = take + paired(give, i, False).astype(f32)
            four = two + paired(two.astype(bf16), i, True).astype(f32)
            summed.append(four.astype(bf16))
        own_cols.append(jnp.concatenate(summed, 0))
        other_cols.append(flipped(jnp.concatenate(summed[::-1], 0), 0))
    projected = jnp.concatenate(own_cols + other_cols, 2)

    flat_proj = projected.reshape(4 * block, -1)
    screened = [lax.dot_general(flat_proj, m, nt, preferred_element_type=f32) for m in screens]
    picked = lax.dot_general(flat_proj, pick, nt, preferred_element_type=f32).astype(bf16)
    batched = (((2,), (2,)), ((0,), (0,)))

    def two_parts(a):
        high = lax.reduce_precision(a, 8, 7)
        return high.astype(bf16), (a - high).astype(bf16)

    block_sigma = sum(
        lax.dot_general(
            part.reshape(4, block, -1),
            picked[:, i * 384 : (i + 1) * 384].reshape(4, block, -1),
            batched,
            preferred_element_type=f32,
        )
        for i, s in enumerate(screened)
        for part in two_parts(s)
    )

    spare_meta = jnp.stack([window_start[last], slot_band[last]])
    got_meta = flipped(spare_meta, 5)
    own_meta = jnp.stack([window_start[:last], slot_band[:last]])
    is_last = jnp.arange(last)[None, :] == last - 1
    meta = jnp.where(is_last & taking, got_meta[:, None], own_meta)
    other_meta = flipped(meta, 0)
    four_meta = jnp.concatenate(
        [
            lax.dynamic_slice_in_dim(m, jnp.where(low[i], 0, 2), 2, 1)
            for i, m in enumerate((meta, other_meta))
        ],
        1,
    )
    starts, band_ids = four_meta[0], four_meta[1]
    band_list = jnp.arange(occupation.shape[0], dtype=jnp.int32)
    weights = 0.5 - jnp.sum(
        jnp.where(band_list[None, :] == band_ids[:, None], occupation[None, :], 0.0), axis=1
    )
    weighted = block_sigma * weights[:, None, None]
    place_rows = (
        jnp.arange(NB_SIGMA, dtype=jnp.int32)[None, :, None] == (starts[:, None] + row_ids)[:, None, :]
    ).astype(bf16)
    sigma_part = sum(
        lax.dot_general(
            lax.dot_general(
                place_rows, w, (((2,), (1,)), ((0,), (0,))), preferred_element_type=f32
            ).astype(bf16),
            place_rows,
            (((0, 2), (0, 2)), ((), ())),
            preferred_element_type=f32,
        )
        for w in two_parts(weighted)
    )
    by_band = lax.all_to_all(
        sigma_part.astype(bf16).reshape(64, 8, NB_SIGMA), "band", 0, 0, tiled=True
    )
    rows = jnp.sum(by_band.astype(f32), axis=0).reshape(4, 2, NB_SIGMA)
    return rows_to_owner(rows, me, core)


def solution(mesh):
    return jax.shard_map(
        body,
        mesh=mesh,
        in_specs=(
            P("band", None, "pw"),
            P("band", "pw"),
            P("pw", None),
            P(),
            P("band"),
            P("band"),
            P("band"),
        ),
        out_specs=P(("band", "pw"), None),
        check_vma=False,
    )
```
